32 devices in a mesh: seq: 8 (over z, core), tp: 4 (over y, x).
Axes of the slice: x: 2, y: 2, z: 4, core: 2. Of those that a mesh axis runs over, the one named last changes fastest.
Arguments:
- tokens: bfloat16 [2048, 4608], P('seq', 'tp'), may hold values from -6 to 6
- attention_gain: float32 [4608], replicated, may hold values from 0.25 to 1.75
- query_weight: bfloat16 [4608, 4096], P(None, 'tp'), may hold values from -0.09375 to 0.09375
- key_weight: bfloat16 [4608, 2048], P(None, 'tp'), may hold values from -0.09375 to 0.09375
- value_weight: bfloat16 [4608, 2048], P(None, 'tp'), may hold values from -0.09375 to 0.09375
- output_weight: bfloat16 [4096, 4608], P('tp'), may hold values from -0.09375 to 0.09375
- post_gain: float32 [4608], replicated, may hold values from 0.25 to 1.75
- local_gain: float32 [4608], replicated, may hold values from 0.25 to 1.75
- local_query_weight: bfloat16 [4608, 4096], P(None, 'tp'), may hold values from -0.09375 to 0.09375
- local_key_weight: bfloat16 [4608, 2048], P(None, 'tp'), may hold values from -0.09375 to 0.09375
- local_value_weight: bfloat16 [4608, 2048], P(None, 'tp'), may hold values from -0.09375 to 0.09375
Outputs:
- hidden: bfloat16 [2048, 4608], P('seq', 'tp')
- local_heads: bfloat16 [2048, 4096], P('seq', 'tp')
The draws below stay inside these ranges and needn't reach their ends.
All inputs are finite; a program needn't handle non-finite values.
Results may differ from the reference program's by a relative error of at most 0.02.
Values may be sent and summed in bfloat16 or wider, within the bound.
A program may use at most 128 MiB of HBM per device.

```python
import jax
import jax.numpy as jnp
from jax import lax

D = 4608
HEADS = 32
KV_HEADS = 16
HEAD_DIM = 128
WINDOW = 128
TOKENS = 2048


def block_scale(stream_key, dims, shards, least, largest):
    level, own = 1.0, jax.random.fold_in(stream_key, 6)
    for dim, blocks in shards:
        heights = jnp.exp(jax.random.uniform(jax.random.fold_in(own, dim), (blocks,), jnp.float32, least / len(shards), largest / len(shards)))
        level = level * jnp.repeat(heights, dims[dim] // blocks).reshape([-1 if axis == dim else 1 for axis in range(len(dims))])
    return level


def centred(rng, dims, deviation, bound, shards=(), held_as=jnp.bfloat16):
    values = jax.random.normal(rng, dims, jnp.float32) * deviation
    if len(shards) > 0:
        values = block_scale(rng, dims, shards, -0.22, 0.18) * values
    return jnp.clip(values, min=-bound, max=bound).astype(held_as)


def setup_inputs(seed: int = 0) -> dict:
    arg_keys = jax.random.split(jax.random.key(seed), 12)
    return {
        "tokens": centred(arg_keys[0], (TOKENS, D), 1.0, 6.0, ((0, 8), (1, 4))),
        "attention_gain": jnp.clip(1.0 + 0.15 * jax.random.normal(arg_keys[1], (D,), jnp.float32), 0.25, 1.75),
        "query_weight": centred(arg_keys[2], (D, HEADS * HEAD_DIM), D ** -0.5, 0.09375, ((1, 4),)),
        "key_weight": centred(arg_keys[3], (D, KV_HEADS * HEAD_DIM), D ** -0.5, 0.09375, ((1, 4),)),
        "value_weight": centred(arg_keys[4], (D, KV_HEADS * HEAD_DIM), D ** -0.5, 0.09375, ((1, 4),)),
        "output_weight": centred(arg_keys[5], (HEADS * HEAD_DIM, D), (HEADS * HEAD_DIM) ** -0.5, 0.09375, ((0, 4),)),
        "post_gain": jnp.clip(1.0 + 0.15 * jax.random.normal(arg_keys[6], (D,), jnp.float32), 0.25, 1.75),
        "local_gain": jnp.clip(1.0 + 0.15 * jax.random.normal(arg_keys[7], (D,), jnp.float32), 0.25, 1.75),
        "local_query_weight": centred(arg_keys[8], (D, HEADS * HEAD_DIM), D ** -0.5, 0.09375, ((1, 4),)),
        "local_key_weight": centred(arg_keys[9], (D, KV_HEADS * HEAD_DIM), D ** -0.5, 0.09375, ((1, 4),)),
        "local_value_weight": centred(arg_keys[10], (D, KV_HEADS * HEAD_DIM), D ** -0.5, 0.09375, ((1, 4),)),
    }


SOFT_CAP = 50.0
NORM_EPS = 1e-06

def rms_scaled(values, weights):
    widened = values.astype(jnp.float32)
    factor = lax.rsqrt(lax.optimization_barrier(jnp.mean(widened * widened, axis=-1, keepdims=True)) + NORM_EPS)
    return widened * factor * weights.astype(jnp.float32)

def rotate(vectors, places):
    head_size = vectors.shape[-1]
    halfway = head_size // 2
    exponents = jnp.arange(halfway, dtype=jnp.float32) * (2.0 / head_size)
    frequency = jnp.power(jnp.float32(10000.0), -exponents)
    angles = places.astype(jnp.float32)[:, None] * frequency[None, :]
    cosine_part = jnp.cos(angles)[:, None, :]
    sine_part = jnp.sin(angles)[:, None, :]
    first_half = vectors[..., :halfway]
    second_half = vectors[..., halfway:]
    return jnp.concatenate([first_half * cosine_part - second_half * sine_part, second_half * cosine_part + first_half * sine_part], axis=-1)

def project_heads(normed, weight_query, weight_key, weight_value, places):
    row_count = normed.shape[0]
    queries = jnp.dot(normed, weight_query, preferred_element_type=jnp.float32).reshape(row_count, -1, HEAD_DIM)
    key_heads = jnp.dot(normed, weight_key, preferred_element_type=jnp.float32).reshape(row_count, -1, HEAD_DIM)
    value_heads = jnp.dot(normed, weight_value, preferred_element_type=jnp.float32).reshape(row_count, -1, HEAD_DIM)
    return (rotate(queries, places).astype(jnp.bfloat16), rotate(key_heads, places).astype(jnp.bfloat16), value_heads.astype(jnp.bfloat16))

def attention(queries, key_heads, value_heads, window_size):
    row_count = queries.shape[0]
    groups = HEADS // KV_HEADS
    grouped = jnp.transpose(queries.reshape(row_count, KV_HEADS, groups, HEAD_DIM), (1, 0, 2, 3))
    keys_first = jnp.transpose(key_heads, (1, 0, 2))
    values_first = jnp.transpose(value_heads, (1, 0, 2))
    places = jnp.arange(row_count, dtype=jnp.int32)
    offset = places[:, None] - places[None, :]
    allowed = (offset >= 0) & (offset < window_size)
    scale = float(D // HEADS) ** (-0.5)

    def one_head(operands):
        query_block, key_block, value_block = operands
        scores = jnp.einsum('qrd,kd->rqk', query_block.astype(jnp.float32), key_block.astype(jnp.float32)) * scale
        scores = SOFT_CAP * jnp.tanh(scores / SOFT_CAP)
        weights = jnp.where(allowed[None], jnp.exp(scores), jnp.float32(0.0))
        denominator = lax.optimization_barrier(jnp.sum(weights, axis=-1))
        probs = weights.astype(jnp.bfloat16)
        numerator = jnp.einsum('rqk,kd->qrd', probs.astype(jnp.float32), value_block.astype(jnp.float32))
        return (numerator / jnp.transpose(denominator)[:, :, None]).astype(jnp.bfloat16)
    stacked = lax.map(one_head, (grouped, keys_first, values_first))
    return jnp.transpose(stacked, (1, 0, 2, 3)).reshape(row_count, HEADS * HEAD_DIM)

def reference(tokens, attention_gain, query_weight, key_weight, value_weight, output_weight, post_gain, local_gain, local_query_weight, local_key_weight, local_value_weight):
    places = jnp.arange(TOKENS, dtype=jnp.int32)
    normed = rms_scaled(tokens, attention_gain).astype(jnp.bfloat16)
    queries, key_heads, value_heads = project_heads(normed, query_weight, key_weight, value_weight, places)
    attended = attention(queries, key_heads, value_heads, TOKENS)
    projected = jnp.dot(attended, output_weight, preferred_element_type=jnp.float32)
    hidden = (tokens.astype(jnp.float32) + rms_scaled(projected, post_gain)).astype(jnp.bfloat16)
    local_normed = rms_scaled(hidden, local_gain).astype(jnp.bfloat16)
    local_queries, local_keys, local_values = project_heads(local_normed, local_query_weight, local_key_weight, local_value_weight, places)
    local_heads = attention(local_queries, local_keys, local_values, WINDOW)
    return (hidden, local_heads)
```

```python
import functools
import math

import jax
import jax.numpy as jnp
from jax import lax
from jax.experimental import pallas as pl
from jax.experimental.pallas import tpu as pltpu
from jax.sharding import PartitionSpec as P

D = 4608
HEADS = 32
HEAD_DIM = 128
WINDOW = 128

SOFT_CAP = 50.0
NORM_EPS = 1e-06
MESH = pl.DeviceIdType.MESH
VMEM = pltpu.VMEM
F32 = jnp.float32
BF16 = jnp.bfloat16
INNER = float(D // HEADS) ** (-0.5) / SOFT_CAP
OUTER = SOFT_CAP * math.log2(math.e)


def greet(peers):
    barrier = pltpu.get_barrier_semaphore()
    for peer in peers:
        pl.semaphore_signal(barrier, inc=1, device_id=peer, device_id_type=MESH)
    pl.semaphore_wait(barrier, len(peers))


def remote(source, target, send_sem, recv_sem, device):
    return pltpu.make_async_remote_copy(
        src_ref=source,
        dst_ref=target,
        send_sem=send_sem,
        recv_sem=recv_sem,
        device_id=device,
        device_id_type=MESH,
    )


def xor(index, bits):
    low, high = index % 2, index // 2
    if bits & 1:
        low = 1 - low
    if bits & 2:
        high = 1 - high
    return high * 2 + low


def gather_project_kernel(
    heads, kv_heads, x_ref, gain_ref, cos_ref, sin_ref, wq_ref, wk_ref, wv_ref,
    q_ref, kv_ref, buf, xg, w, acc, ss, send, recv, wsem,
):
    me = lax.axis_index("tp")
    rows, cols = x_ref.shape
    half = rows // 2
    owners = [xor(me, bits) for bits in range(4)]
    along_x, along_y = {"tp": owners[1]}, {"tp": owners[2]}
    qc, kc = heads * HEAD_DIM, kv_heads * HEAD_DIM
    total = qc + 2 * kc

    loads = []
    for slot in range(4):
        span = pl.ds(pl.multiple_of(owners[slot] * cols, cols), cols)
        parts = ((wq_ref, 0, qc), (wk_ref, qc, kc), (wv_ref, qc + kc, kc))
        group = []
        for which, (ref, begin, width) in enumerate(parts):
            copy = pltpu.make_async_copy(
                ref.at[span, :], w.at[slot, :, pl.ds(begin, width)], wsem.at[slot, which]
            )
            copy.start()
            group.append(copy)
        loads.append(group)

    greet([along_x, along_y])
    top, bottom = pl.ds(0, half), pl.ds(half, half)
    x_top = remote(x_ref.at[top], buf.at[0, top], send.at[0], recv.at[0], along_x)
    y_bottom = remote(x_ref.at[bottom], buf.at[1, bottom], send.at[1], recv.at[1], along_y)
    x_bottom = remote(x_ref.at[bottom], buf.at[0, bottom], send.at[2], recv.at[2], along_x)
    y_top = remote(x_ref.at[top], buf.at[1, top], send.at[3], recv.at[3], along_y)
    pass_y = remote(buf.at[0, top], buf.at[2, top], send.at[4], recv.at[4], along_y)
    pass_x = remote(buf.at[1, bottom], buf.at[2, bottom], send.at[5], recv.at[5], along_x)
    x_top.start()
    y_bottom.start()
    x_bottom.start()
    y_top.start()

    tile = 256 if total % 256 == 0 else 128
    step_rows = 64 if rows % 64 == 0 else rows

    def take(slot, source):
        gain_span = pl.ds(pl.multiple_of(owners[slot] * cols, cols), cols)

        def prepare(i, carry):
            part = pl.ds(pl.multiple_of(i * step_rows, step_rows), step_rows)
            wide = source[part, :].astype(F32)
            squares = jnp.sum(wide * wide, axis=-1, keepdims=True)
            spread = jnp.broadcast_to(squares, (step_rows, HEAD_DIM))
            if slot == 0:
                ss[part, :] = spread
            else:
                ss[part, :] += spread
            xg[part, :] = (wide * gain_ref[:, gain_span]).astype(BF16)
            return carry

        lax.fori_loop(0, rows // step_rows, prepare, 0)
        for copy in loads[slot]:
            copy.wait()

        def multiply(j, carry):
            span = pl.ds(pl.multiple_of(j * tile, tile), tile)
            product = jnp.dot(xg[...], w[slot, :, span], preferred_element_type=F32)
            if slot == 0:
                acc[:, span] = product
            else:
                acc[:, span] += product
            return carry

        lax.fori_loop(0, total // tile, multiply, 0)

    take(0, x_ref)
    x_top.wait_recv()
    pass_y.start()
    y_bottom.wait_recv()
    pass_x.start()
    x_bottom.wait_recv()
    take(1, buf.at[0])
    y_top.wait_recv()
    take(2, buf.at[1])
    pass_y.wait_recv()
    pass_x.wait_recv()
    take(3, buf.at[2])

    factor = lax.rsqrt(ss[...] * (1.0 / D) + NORM_EPS)

    def rotated(index):
        u = acc[:, pl.ds(index * HEAD_DIM, HEAD_DIM)] * factor
        return u * cos_ref[...] + pltpu.roll(u, HEAD_DIM // 2, 1) * sin_ref[...]

    for h in range(heads):
        q_ref[h] = rotated(h).astype(BF16)
    for h in range(kv_heads):
        kv_ref[0, h] = rotated(heads + h).astype(BF16)
        place = (heads + kv_heads + h) * HEAD_DIM
        kv_ref[1, h] = (acc[:, pl.ds(place, HEAD_DIM)] * factor).astype(BF16)
    for copy in (x_top, y_bottom, x_bottom, y_top, pass_y, pass_x):
        copy.wait_send()


def gather_project(x, gain, cos, sin, wq, wk, wv, collective_id):
    rows, cols = x.shape
    heads, kv_heads = wq.shape[1] // HEAD_DIM, wk.shape[1] // HEAD_DIM
    total = wq.shape[1] + 2 * wk.shape[1]
    vmem = pl.BlockSpec(memory_space=VMEM)
    hbm = pl.BlockSpec(memory_space=pl.ANY)
    return pl.pallas_call(
        functools.partial(gather_project_kernel, heads, kv_heads),
        out_shape=(
            jax.ShapeDtypeStruct((heads, rows, HEAD_DIM), BF16),
            jax.ShapeDtypeStruct((2, kv_heads, rows, HEAD_DIM), BF16),
        ),
        in_specs=[vmem] * 4 + [hbm] * 3,
        out_specs=(vmem, vmem),
        scratch_shapes=[
            VMEM((3, rows, cols), BF16),
            VMEM((rows, cols), BF16),
            VMEM((4, cols, total), BF16),
            VMEM((rows, total), F32),
            VMEM((rows, HEAD_DIM), F32),
            pltpu.SemaphoreType.DMA((6,)),
            pltpu.SemaphoreType.DMA((6,)),
            pltpu.SemaphoreType.DMA((4, 3)),
        ],
        compiler_params=pltpu.CompilerParams(
            collective_id=collective_id, has_side_effects=True, vmem_limit_bytes=48 * 2**20
        ),
        name=f"gather_project_{collective_id}",
    )(x, gain[None, :], cos, sin, wq, wk, wv)


def attend(q_ref, keys, values, acc, lsum, h, group, allowed, first, row_span=None):
    q = q_ref[pl.ds(h * group, group)]
    if row_span is not None:
        q = q[:, row_span[0] : row_span[1]]
    rows = q.shape[1]
    q = q.reshape(group * rows, HEAD_DIM)
    scores = lax.dot_general(q, keys, (((1,), (1,)), ((), ())), preferred_element_type=F32)
    weights = jnp.exp2(jnp.tanh(scores * INNER) * OUTER)
    if allowed is not None:
        count = keys.shape[0]
        row = lax.broadcasted_iota(jnp.int32, (rows, count), 0)
        col = lax.broadcasted_iota(jnp.int32, (rows, count), 1)
        mask = allowed(row, col)
        weights = jnp.concatenate(
            [jnp.where(mask, weights[g * rows : (g + 1) * rows], 0.0) for g in range(group)], axis=0
        )
    lanes = weights[:, :HEAD_DIM]
    for begin in range(HEAD_DIM, keys.shape[0], HEAD_DIM):
        lanes = lanes + weights[:, begin : begin + HEAD_DIM]
    product = jnp.dot(weights.astype(BF16), values, preferred_element_type=F32)
    lanes = lanes.reshape(group, rows, HEAD_DIM)
    product = product.reshape(group, rows, HEAD_DIM)
    heads = pl.ds(h * group, group)
    span = pl.ds(0, rows)
    if first:
        lsum[heads, span] = lanes
        acc[heads, span] = product
    else:
        lsum[heads, span] += lanes
        acc[heads, span] += product


def write_heads(o_ref, acc, lsum):
    for h in range(acc.shape[0]):
        denominator = jnp.sum(lsum[h], axis=-1, keepdims=True)
        o_ref[:, h * HEAD_DIM : (h + 1) * HEAD_DIM] = (acc[h] / denominator).astype(BF16)


def causal_kernel(levels, q_ref, kv_ref, o_ref, buf, acc, lsum, up_sem, side_sem, recv):
    s = lax.axis_index("seq")
    z, c = s // 2, s % 2
    mate = s + 1 - 2 * c
    kv_heads = kv_ref.shape[1]
    group = q_ref.shape[0] // kv_heads
    has_up, has_down = z < levels - 1, z > 0

    barrier = pltpu.get_barrier_semaphore()
    pl.semaphore_signal(barrier, inc=1, device_id={"seq": mate}, device_id_type=MESH)

    @pl.when(has_up)
    def _():
        pl.semaphore_signal(barrier, inc=1, device_id={"seq": s + 2}, device_id_type=MESH)

    @pl.when(has_down)
    def _():
        pl.semaphore_signal(barrier, inc=1, device_id={"seq": s - 2}, device_id_type=MESH)

    pl.semaphore_wait(barrier, 1 + has_up.astype(jnp.int32) + has_down.astype(jnp.int32))

    def up(owner, source):
        return remote(source, buf.at[owner], up_sem.at[owner], recv.at[owner], {"seq": s + 2})

    def side(owner, source):
        return remote(source, buf.at[owner], side_sem.at[owner], recv.at[owner], {"seq": mate})

    @pl.when(has_up)
    def _():
        up(s, kv_ref).start()

    @pl.when(c == 0)
    def _():
        side(s, kv_ref).start()

    def own(h, carry):
        attend(
            q_ref, kv_ref[0, h], kv_ref[1, h], acc, lsum, h, group,
            lambda row, col: col <= row, True,
        )
        return carry

    lax.fori_loop(0, kv_heads, own, 0)

    def visit(owner):
        def body(h, carry):
            attend(
                q_ref, buf[owner, 0, h], buf[owner, 1, h], acc, lsum, h, group, None, False
            )
            return carry

        lax.fori_loop(0, kv_heads, body, 0)

    @pl.when(c == 1)
    def _():
        side(s - 1, buf.at[s - 1]).wait_recv()
        visit(s - 1)

    def level(k, carry):
        owner, other = s - 2 * k, mate - 2 * k
        up(owner, buf.at[owner]).wait_recv()

        @pl.when(has_up)
        def _():
            up(owner, buf.at[owner]).start()

        side(owner, buf.at[owner]).start()
        visit(owner)
        side(other, buf.at[other]).wait_recv()
        visit(other)
        return carry

    lax.fori_loop(1, z + 1, level, 0)
    write_heads(o_ref, acc, lsum)

    @pl.when(has_up)
    def _():
        up(s, kv_ref).wait_send()

    @pl.when(c == 0)
    def _():
        side(s, kv_ref).wait_send()

    def drain(k, carry):
        owner = s - 2 * k

        @pl.when(has_up)
        def _():
            up(owner, buf.at[owner]).wait_send()

        side(owner, buf.at[owner]).wait_send()
        return carry

    lax.fori_loop(1, z + 1, drain, 0)


def causal_attention(q, kv, count, collective_id):
    heads, rows, _ = q.shape
    vmem = pl.BlockSpec(memory_space=VMEM)
    return pl.pallas_call(
        functools.partial(causal_kernel, count // 2),
        out_shape=jax.ShapeDtypeStruct((rows, heads * HEAD_DIM), BF16),
        in_specs=[vmem] * 2,
        out_specs=vmem,
        scratch_shapes=[
            VMEM((count,) + kv.shape, BF16),
            VMEM(q.shape, F32),
            VMEM(q.shape, F32),
            pltpu.SemaphoreType.DMA((count,)),
            pltpu.SemaphoreType.DMA((count,)),
            pltpu.SemaphoreType.DMA((count,)),
        ],
        compiler_params=pltpu.CompilerParams(
            collective_id=collective_id, has_side_effects=True, vmem_limit_bytes=32 * 2**20
        ),
        name="causal_attention",
    )(q, kv)


def output_kernel(
    a_ref, tok_ref, gain_ref, wo_ref, hidden_ref,
    wbuf, part, own, landed, passed, mine, stats, wsem, send, recv, ssend, srecv,
):
    me = lax.axis_index("tp")
    rows, cols = tok_ref.shape
    half = rows // 2
    owners = [xor(me, bits) for bits in range(4)]
    peers = [{"tp": owner} for owner in owners]
    order = (3, 1, 2, 0)
    loads = []
    for slot, bits in enumerate(order):
        span = pl.ds(pl.multiple_of(owners[bits] * cols, cols), cols)
        copy = pltpu.make_async_copy(wo_ref.at[:, span], wbuf.at[slot], wsem.at[slot])
        copy.start()
        loads.append(copy)
    greet(peers[1:])
    top, bottom = pl.ds(0, half), pl.ds(half, half)
    diag_x = remote(part.at[0, top], landed.at[0], send.at[0], recv.at[0], peers[1])
    diag_y = remote(part.at[0, bottom], landed.at[1], send.at[1], recv.at[1], peers[2])
    last_x_top = remote(part.at[1, top], landed.at[2], send.at[2], recv.at[2], peers[1])
    last_y_bottom = remote(part.at[2, bottom], landed.at[3], send.at[3], recv.at[3], peers[2])
    last_x_bottom = remote(passed.at[1], landed.at[4], send.at[4], recv.at[4], peers[1])
    last_y_top = remote(passed.at[0], landed.at[5], send.at[5], recv.at[5], peers[2])

    tile = 384 if cols % 384 == 0 else 128

    def product(slot, store):
        loads[slot].wait()

        def body(j, carry):
            span = pl.ds(pl.multiple_of(j * tile, tile), tile)
            store(span, jnp.dot(a_ref[...], wbuf[slot, :, span], preferred_element_type=F32))
            return carry

        lax.fori_loop(0, cols // tile, body, 0)

    def store_part(slot):
        def store(span, value):
            part[slot, :, span] = value.astype(BF16)

        return store

    def store_own(span, value):
        own[:, span] = value

    product(0, store_part(0))
    diag_x.start()
    diag_y.start()
    product(1, store_part(1))
    last_x_top.start()
    product(2, store_part(2))
    last_y_bottom.start()
    product(3, store_own)
    diag_x.wait_recv()
    passed[0] = (part[2, 0:half].astype(F32) + landed[0].astype(F32)).astype(BF16)
    last_y_top.start()
    diag_y.wait_recv()
    passed[1] = (part[1, half:rows].astype(F32) + landed[1].astype(F32)).astype(BF16)
    last_x_bottom.start()
    last_x_top.wait_recv()
    own[0:half] += landed[2].astype(F32)
    last_y_bottom.wait_recv()
    own[half:rows] += landed[3].astype(F32)
    last_y_top.wait_recv()
    own[0:half] += landed[5].astype(F32)
    last_x_bottom.wait_recv()
    own[half:rows] += landed[4].astype(F32)

    lanes = jnp.zeros((rows, HEAD_DIM), F32)
    for begin in range(0, cols, HEAD_DIM):
        piece = own[:, begin : begin + HEAD_DIM]
        lanes = lanes + piece * piece
    ones = jnp.ones((8, HEAD_DIM), F32)
    highest = lax.Precision.HIGHEST
    mine[...] = lax.dot_general(
        ones, lanes, (((1,), (1,)), ((), ())), precision=highest, preferred_element_type=F32
    )
    swaps = []
    for bits in (3, 1, 2):
        swap = remote(mine, stats.at[bits - 1], ssend.at[bits - 1], srecv.at[bits - 1], peers[bits])
        swap.start()
        swaps.append(swap)
    for swap in swaps:
        swap.wait_recv()
    summed = mine[...] + stats[0] + stats[1] + stats[2]
    column = lax.dot_general(
        summed, ones * 0.125, (((0,), (0,)), ((), ())), precision=highest,
        preferred_element_type=F32,
    )
    factor = lax.rsqrt(column * (1.0 / D) + NORM_EPS)
    span = pl.multiple_of(me * cols, cols)
    for begin in range(0, cols, HEAD_DIM):
        stop = begin + HEAD_DIM
        gain = gain_ref[:, pl.ds(pl.multiple_of(span + begin, HEAD_DIM), HEAD_DIM)]
        hidden_ref[:, begin:stop] = (
            tok_ref[:, begin:stop].astype(F32) + own[:, begin:stop] * factor * gain
        ).astype(BF16)
    for copy in (diag_x, diag_y, last_x_top, last_y_bottom, last_x_bottom, last_y_top, *swaps):
        copy.wait_send()


def output_project(attended, tokens, gain, wo, collective_id):
    rows, cols = tokens.shape
    depth = attended.shape[1]
    vmem = pl.BlockSpec(memory_space=VMEM)
    return pl.pallas_call(
        output_kernel,
        out_shape=jax.ShapeDtypeStruct((rows, cols), BF16),
        in_specs=[vmem] * 3 + [pl.BlockSpec(memory_space=pl.ANY)],
        out_specs=vmem,
        scratch_shapes=[
            VMEM((4, depth, cols), BF16),
            VMEM((3, rows, cols), BF16),
            VMEM((rows, cols), F32),
            VMEM((6, rows // 2, cols), BF16),
            VMEM((2, rows // 2, cols), BF16),
            VMEM((8, rows), F32),
            VMEM((3, 8, rows), F32),
            pltpu.SemaphoreType.DMA((4,)),
            pltpu.SemaphoreType.DMA((6,)),
            pltpu.SemaphoreType.DMA((6,)),
            pltpu.SemaphoreType.DMA((3,)),
            pltpu.SemaphoreType.DMA((3,)),
        ],
        compiler_params=pltpu.CompilerParams(
            collective_id=collective_id, has_side_effects=True, vmem_limit_bytes=40 * 2**20
        ),
        name="output_project",
    )(attended, tokens, gain[None, :], wo)


def window_kernel(count, q_ref, kv_ref, o_ref, tail, acc, lsum, send, recv):
    s = lax.axis_index("seq")
    kv_heads, rows = kv_ref.shape[1], kv_ref.shape[2]
    group = q_ref.shape[0] // kv_heads
    has_next, has_last = s < count - 1, s > 0
    barrier = pltpu.get_barrier_semaphore()

    @pl.when(has_next)
    def _():
        pl.semaphore_signal(barrier, inc=1, device_id={"seq": s + 1}, device_id_type=MESH)

    @pl.when(has_last)
    def _():
        pl.semaphore_signal(barrier, inc=1, device_id={"seq": s - 1}, device_id_type=MESH)

    pl.semaphore_wait(barrier, has_next.astype(jnp.int32) + has_last.astype(jnp.int32))
    copy = remote(
        kv_ref.at[:, :, pl.ds(rows - WINDOW, WINDOW), :], tail, send.at[0], recv.at[0],
        {"seq": s + 1},
    )

    @pl.when(has_next)
    def _():
        copy.start()

    def own(h, carry):
        attend(
            q_ref, kv_ref[0, h], kv_ref[1, h], acc, lsum, h, group,
            lambda row, col: (col <= row) & (row - col < WINDOW), True,
        )
        return carry

    lax.fori_loop(0, kv_heads, own, 0)

    @pl.when(has_last)
    def _():
        copy.wait_recv()

        def body(h, carry):
            attend(
                q_ref, tail[0, h], tail[1, h], acc, lsum, h, group,
                lambda row, col: col > row, False, (0, WINDOW),
            )
            return carry

        lax.fori_loop(0, kv_heads, body, 0)

    write_heads(o_ref, acc, lsum)

    @pl.when(has_next)
    def _():
        copy.wait_send()


def window_attention(q, kv, count, collective_id):
    heads, rows, _ = q.shape
    vmem = pl.BlockSpec(memory_space=VMEM)
    return pl.pallas_call(
        functools.partial(window_kernel, count),
        out_shape=jax.ShapeDtypeStruct((rows, heads * HEAD_DIM), BF16),
        in_specs=[vmem] * 2,
        out_specs=vmem,
        scratch_shapes=[
            VMEM((2, kv.shape[1], WINDOW, HEAD_DIM), BF16),
            VMEM(q.shape, F32),
            VMEM(q.shape, F32),
            pltpu.SemaphoreType.DMA((1,)),
            pltpu.SemaphoreType.DMA((1,)),
        ],
        compiler_params=pltpu.CompilerParams(
            collective_id=collective_id, has_side_effects=True, vmem_limit_bytes=24 * 2**20
        ),
        name="window_attention",
    )(q, kv)


def rms_scaled(values, weights):
    widened = values.astype(F32)
    factor = lax.rsqrt(jnp.mean(widened * widened, axis=-1, keepdims=True) + NORM_EPS)
    return widened * factor * weights


def plain_gather_project(x, gain, cos, sin, wq, wk, wv):
    full = lax.all_gather(x, "tp", axis=1, tiled=True)
    normed = rms_scaled(full, gain).astype(BF16)

    def heads_of(weight):
        product = jnp.dot(normed, weight, preferred_element_type=F32)
        return jnp.swapaxes(product.reshape(x.shape[0], -1, HEAD_DIM), 0, 1)

    def rotated(u):
        return (u * cos + jnp.roll(u, HEAD_DIM // 2, axis=-1) * sin).astype(BF16)

    keys, values = rotated(heads_of(wk)), heads_of(wv).astype(BF16)
    return rotated(heads_of(wq)), jnp.stack([keys, values])


def plain_output_project(attended, tokens, gain, wo):
    cols = tokens.shape[1]
    partial_sum = jnp.dot(attended, wo, preferred_element_type=F32).astype(BF16)
    summed = lax.psum(partial_sum, "tp").astype(F32)
    added = rms_scaled(summed, gain)
    mine = lax.dynamic_slice_in_dim(added, lax.axis_index("tp") * cols, cols, 1)
    return (tokens.astype(F32) + mine).astype(BF16)


def local(
    sizes,
    tokens,
    attention_gain,
    query_weight,
    key_weight,
    value_weight,
    output_weight,
    post_gain,
    local_gain,
    local_query_weight,
    local_key_weight,
    local_value_weight,
):
    seq, tp = sizes
    rows, cols = tokens.shape
    places = lax.axis_index("seq") * rows + lax.iota(jnp.int32, rows)
    halfway = HEAD_DIM // 2
    exponents = jnp.arange(halfway, dtype=F32) * (2.0 / HEAD_DIM)
    frequency = jnp.power(F32(10000.0), -exponents)
    angles = places.astype(F32)[:, None] * frequency[None, :]
    cosine, sine = jnp.cos(angles), jnp.sin(angles)
    cos = jnp.concatenate([cosine, cosine], axis=-1)
    sin = jnp.concatenate([-sine, sine], axis=-1)
    square = tp == 4 and cols % HEAD_DIM == 0

    def project(x, gain, wq, wk, wv, collective_id):
        if square:
            return gather_project(x, gain, cos, sin, wq, wk, wv, collective_id)
        return plain_gather_project(x, gain, cos, sin, wq, wk, wv)

    q, kv = project(tokens, attention_gain, query_weight, key_weight, value_weight, 0)
    attended = causal_attention(q, kv, seq, 1)
    if square:
        hidden = output_project(attended, tokens, post_gain, output_weight, 2)
    else:
        hidden = plain_output_project(attended, tokens, post_gain, output_weight)
    lq, lkv = project(
        hidden, local_gain, local_query_weight, local_key_weight, local_value_weight, 3
    )
    return hidden, window_attention(lq, lkv, seq, 4)


def solution(mesh):
    in_specs = (
        P("seq", "tp"),
        P(),
        P(None, "tp"),
        P(None, "tp"),
        P(None, "tp"),
        P("tp", None),
        P(),
        P(),
        P(None, "tp"),
        P(None, "tp"),
        P(None, "tp"),
    )
    out_specs = (P("seq", "tp"), P("seq", "tp"))
    sizes = (mesh.shape["seq"], mesh.shape["tp"])
    body = functools.partial(local, sizes)
    return jax.shard_map(body, mesh=mesh, in_specs=in_specs, out_specs=out_specs, check_vma=False)
```

```python
import functools
import math

import jax
import jax.numpy as jnp
from jax import lax
from jax.experimental import pallas as pl
from jax.experimental.pallas import tpu as pltpu
from jax.sharding import PartitionSpec as P

D = 4608
HEADS = 32
HEAD_DIM = 128
WINDOW = 128

SOFT_CAP = 50.0
NORM_EPS = 1e-06
MESH = pl.DeviceIdType.MESH
VMEM = pltpu.VMEM
F32 = jnp.float32
BF16 = jnp.bfloat16
INNER = float(D // HEADS) ** (-0.5) / SOFT_CAP
OUTER = SOFT_CAP * math.log2(math.e)


def greet(peers):
    barrier = pltpu.get_barrier_semaphore()
    for peer in peers:
        pl.semaphore_signal(barrier, inc=1, device_id=peer, device_id_type=MESH)
    pl.semaphore_wait(barrier, len(peers))


def remote(source, target, send_sem, recv_sem, device):
    return pltpu.make_async_remote_copy(
        src_ref=source,
        dst_ref=target,
        send_sem=send_sem,
        recv_sem=recv_sem,
        device_id=device,
        device_id_type=MESH,
    )


def xor(index, bits):
    low, high = index % 2, index // 2
    if bits & 1:
        low = 1 - low
    if bits & 2:
        high = 1 - high
    return high * 2 + low


def gather_project_kernel(
    heads, kv_heads, x_ref, gain_ref, cos_ref, sin_ref, wq_ref, wk_ref, wv_ref,
    q_ref, kv_ref, buf, xg, w, acc, ss, send, recv, wsem,
):
    me = lax.axis_index("tp")
    rows, cols = x_ref.shape
    half = rows // 2
    owners = [xor(me, bits) for bits in range(4)]
    along_x, along_y = {"tp": owners[1]}, {"tp": owners[2]}
    qc, kc = heads * HEAD_DIM, kv_heads * HEAD_DIM
    total = qc + 2 * kc

    loads = []
    for slot in range(4):
        span = pl.ds(pl.multiple_of(owners[slot] * cols, cols), cols)
        parts = ((wq_ref, 0, qc), (wk_ref, qc, kc), (wv_ref, qc + kc, kc))
        group = []
        for which, (ref, begin, width) in enumerate(parts):
            copy = pltpu.make_async_copy(
                ref.at[span, :], w.at[slot, :, pl.ds(begin, width)], wsem.at[slot, which]
            )
            copy.start()
            group.append(copy)
        loads.append(group)

    greet([along_x, along_y])
    top, bottom = pl.ds(0, half), pl.ds(half, half)
    x_top = remote(x_ref.at[top], buf.at[0, top], send.at[0], recv.at[0], along_x)
    y_bottom = remote(x_ref.at[bottom], buf.at[1, bottom], send.at[1], recv.at[1], along_y)
    x_bottom = remote(x_ref.at[bottom], buf.at[0, bottom], send.at[2], recv.at[2], along_x)
    y_top = remote(x_ref.at[top], buf.at[1, top], send.at[3], recv.at[3], along_y)
    pass_y = remote(buf.at[0, top], buf.at[2, top], send.at[4], recv.at[4], along_y)
    pass_x = remote(buf.at[1, bottom], buf.at[2, bottom], send.at[5], recv.at[5], along_x)
    x_top.start()
    y_bottom.start()
    x_bottom.start()
    y_top.start()

    tile = 256 if total % 256 == 0 else 128
    step_rows = 64 if rows % 64 == 0 else rows

    def take(slot, source):
        gain_span = pl.ds(pl.multiple_of(owners[slot] * cols, cols), cols)

        def prepare(i, carry):
            part = pl.ds(pl.multiple_of(i * step_rows, step_rows), step_rows)
            wide = source[part, :].astype(F32)
            squares = jnp.sum(wide * wide, axis=-1, keepdims=True)
            spread = jnp.broadcast_to(squares, (step_rows, HEAD_DIM))
            if slot == 0:
                ss[part, :] = spread
            else:
                ss[part, :] += spread
            xg[part, :] = (wide * gain_ref[:, gain_span]).astype(BF16)
            return carry

        lax.fori_loop(0, rows // step_rows, prepare, 0)
        for copy in loads[slot]:
            copy.wait()

        def multiply(j, carry):
            span = pl.ds(pl.multiple_of(j * tile, tile), tile)
            product = jnp.dot(xg[...], w[slot, :, span], preferred_element_type=F32)
            if slot == 0:
                acc[:, span] = product
            else:
                acc[:, span] += product
            return carry

        lax.fori_loop(0, total // tile, multiply, 0)

    take(0, x_ref)
    x_top.wait_recv()
    pass_y.start()
    y_bottom.wait_recv()
    pass_x.start()
    x_bottom.wait_recv()
    take(1, buf.at[0])
    y_top.wait_recv()
    take(2, buf.at[1])
    pass_y.wait_recv()
    pass_x.wait_recv()
    take(3, buf.at[2])

    factor = lax.rsqrt(ss[...] * (1.0 / D) + NORM_EPS)

    def rotated(index):
        u = acc[:, pl.ds(index * HEAD_DIM, HEAD_DIM)] * factor
        return u * cos_ref[...] + pltpu.roll(u, HEAD_DIM // 2, 1) * sin_ref[...]

    for h in range(heads):
        q_ref[h] = rotated(h).astype(BF16)
    for h in range(kv_heads):
        kv_ref[0, h] = rotated(heads + h).astype(BF16)
        place = (heads + kv_heads + h) * HEAD_DIM
        kv_ref[1, h] = (acc[:, pl.ds(place, HEAD_DIM)] * factor).astype(BF16)
    for copy in (x_top, y_bottom, x_bottom, y_top, pass_y, pass_x):
        copy.wait_send()


def gather_project(x, gain, cos, sin, wq, wk, wv, collective_id):
    rows, cols = x.shape
    heads, kv_heads = wq.shape[1] // HEAD_DIM, wk.shape[1] // HEAD_DIM
    total = wq.shape[1] + 2 * wk.shape[1]
    vmem = pl.BlockSpec(memory_space=VMEM)
    hbm = pl.BlockSpec(memory_space=pl.ANY)
    return pl.pallas_call(
        functools.partial(gather_project_kernel, heads, kv_heads),
        out_shape=(
            jax.ShapeDtypeStruct((heads, rows, HEAD_DIM), BF16),
            jax.ShapeDtypeStruct((2, kv_heads, rows, HEAD_DIM), BF16),
        ),
        in_specs=[vmem] * 4 + [hbm] * 3,
        out_specs=(vmem, vmem),
        scratch_shapes=[
            VMEM((3, rows, cols), BF16),
            VMEM((rows, cols), BF16),
            VMEM((4, cols, total), BF16),
            VMEM((rows, total), F32),
            VMEM((rows, HEAD_DIM), F32),
            pltpu.SemaphoreType.DMA((6,)),
            pltpu.SemaphoreType.DMA((6,)),
            pltpu.SemaphoreType.DMA((4, 3)),
        ],
        compiler_params=pltpu.CompilerParams(
            collective_id=collective_id, has_side_effects=True, vmem_limit_bytes=48 * 2**20
        ),
        name=f"gather_project_{collective_id}",
    )(x, gain[None, :], cos, sin, wq, wk, wv)


def attend(q_ref, keys, values, acc, lsum, h, group, allowed, first, row_span=None):
    q = q_ref[pl.ds(h * group, group)]
    if row_span is not None:
        q = q[:, row_span[0] : row_span[1]]
    rows = q.shape[1]
    q = q.reshape(group * rows, HEAD_DIM)
    scores = lax.dot_general(q, keys, (((1,), (1,)), ((), ())), preferred_element_type=F32)
    weights = jnp.exp2(jnp.tanh(scores * INNER) * OUTER)
    if allowed is not None:
        count = keys.shape[0]
        row = lax.broadcasted_iota(jnp.int32, (rows, count), 0)
        col = lax.broadcasted_iota(jnp.int32, (rows, count), 1)
        mask = allowed(row, col)
        weights = jnp.concatenate(
            [jnp.where(mask, weights[g * rows : (g + 1) * rows], 0.0) for g in range(group)], axis=0
        )
    lanes = weights[:, :HEAD_DIM]
    for begin in range(HEAD_DIM, keys.shape[0], HEAD_DIM):
        lanes = lanes + weights[:, begin : begin + HEAD_DIM]
    product = jnp.dot(weights.astype(BF16), values, preferred_element_type=F32)
    lanes = lanes.reshape(group, rows, HEAD_DIM)
    product = product.reshape(group, rows, HEAD_DIM)
    heads = pl.ds(h * group, group)
    span = pl.ds(0, rows)
    if first:
        lsum[heads, span] = lanes
        acc[heads, span] = product
    else:
        lsum[heads, span] += lanes
        acc[heads, span] += product


def write_heads(o_ref, acc, lsum):
    for h in range(acc.shape[0]):
        denominator = jnp.sum(lsum[h], axis=-1, keepdims=True)
        o_ref[:, h * HEAD_DIM : (h + 1) * HEAD_DIM] = (acc[h] / denominator).astype(BF16)


def causal_kernel(levels, q_ref, kv_ref, o_ref, buf, acc, lsum, up_sem, side_sem, recv):
    s = lax.axis_index("seq")
    z, c = s // 2, s % 2
    mate = s + 1 - 2 * c
    kv_heads = kv_ref.shape[1]
    group = q_ref.shape[0] // kv_heads
    has_up, has_down = z < levels - 1, z > 0

    barrier = pltpu.get_barrier_semaphore()
    pl.semaphore_signal(barrier, inc=1, device_id={"seq": mate}, device_id_type=MESH)

    @pl.when(has_up)
    def _():
        pl.semaphore_signal(barrier, inc=1, device_id={"seq": s + 2}, device_id_type=MESH)

    @pl.when(has_down)
    def _():
        pl.semaphore_signal(barrier, inc=1, device_id={"seq": s - 2}, device_id_type=MESH)

    pl.semaphore_wait(barrier, 1 + has_up.astype(jnp.int32) + has_down.astype(jnp.int32))

    def up(owner, source):
        return remote(source, buf.at[owner], up_sem.at[owner], recv.at[owner], {"seq": s + 2})

    def side(owner, source):
        return remote(source, buf.at[owner], side_sem.at[owner], recv.at[owner], {"seq": mate})

    @pl.when(has_up)
    def _():
        up(s, kv_ref).start()

    @pl.when(c == 0)
    def _():
        side(s, kv_ref).start()

    def own(h, carry):
        attend(
            q_ref, kv_ref[0, h], kv_ref[1, h], acc, lsum, h, group,
            lambda row, col: col <= row, True,
        )
        return carry

    lax.fori_loop(0, kv_heads, own, 0)

    def visit(owner):
        def body(h, carry):
            attend(
                q_ref, buf[owner, 0, h], buf[owner, 1, h], acc, lsum, h, group, None, False
            )
            return carry

        lax.fori_loop(0, kv_heads, body, 0)

    @pl.when(c == 1)
    def _():
        side(s - 1, buf.at[s - 1]).wait_recv()
        visit(s - 1)

    def level(k, carry):
        owner, other = s - 2 * k, mate - 2 * k
        up(owner, buf.at[owner]).wait_recv()

        @pl.when(has_up)
        def _():
            up(owner, buf.at[owner]).start()

        side(owner, buf.at[owner]).start()
        visit(owner)
        side(other, buf.at[other]).wait_recv()
        visit(other)
        return carry

    lax.fori_loop(1, z + 1, level, 0)
    write_heads(o_ref, acc, lsum)

    @pl.when(has_up)
    def _():
        up(s, kv_ref).wait_send()

    @pl.when(c == 0)
    def _():
        side(s, kv_ref).wait_send()

    def drain(k, carry):
        owner = s - 2 * k

        @pl.when(has_up)
        def _():
            up(owner, buf.at[owner]).wait_send()

        side(owner, buf.at[owner]).wait_send()
        return carry

    lax.fori_loop(1, z + 1, drain, 0)


def causal_attention(q, kv, count, collective_id):
    heads, rows, _ = q.shape
    vmem = pl.BlockSpec(memory_space=VMEM)
    return pl.pallas_call(
        functools.partial(causal_kernel, count // 2),
        out_shape=jax.ShapeDtypeStruct((rows, heads * HEAD_DIM), BF16),
        in_specs=[vmem] * 2,
        out_specs=vmem,
        scratch_shapes=[
            VMEM((count,) + kv.shape, BF16),
            VMEM(q.shape, F32),
            VMEM(q.shape, F32),
            pltpu.SemaphoreType.DMA((count,)),
            pltpu.SemaphoreType.DMA((count,)),
            pltpu.SemaphoreType.DMA((count,)),
        ],
        compiler_params=pltpu.CompilerParams(
            collective_id=collective_id, has_side_effects=True, vmem_limit_bytes=32 * 2**20
        ),
        name="causal_attention",
    )(q, kv)


def front_kernel(
    levels, heads, kv_heads, x_ref, gain_ref, cos_ref, sin_ref, wq_ref, wk_ref, wv_ref,
    o_ref, buf, xg, w, acc, ss, q_all, kv_own, kv_buf, out, lsum,
    send, recv, wsem, up_sem, side_sem, kv_sem,
):
    me = lax.axis_index("tp")
    s = lax.axis_index("seq")
    z, c = s // 2, s % 2
    mate = s + 1 - 2 * c
    has_up, has_down = z < levels - 1, z > 0
    rows, cols = x_ref.shape
    half, quarter = rows // 2, rows // 4
    owners = [xor(me, bits) for bits in range(4)]
    along_x, along_y = {"tp": owners[1]}, {"tp": owners[2]}
    qc, kc = heads * HEAD_DIM, kv_heads * HEAD_DIM
    total = qc + 2 * kc
    group = heads // kv_heads

    loads = []
    for slot in range(4):
        span = pl.ds(pl.multiple_of(owners[slot] * cols, cols), cols)
        parts = ((wq_ref, 0, qc), (wk_ref, qc, kc), (wv_ref, qc + kc, kc))
        bundle = []
        for which, (ref, begin, width) in enumerate(parts):
            copy = pltpu.make_async_copy(
                ref.at[span, :], w.at[slot, :, pl.ds(begin, width)], wsem.at[slot, which]
            )
            copy.start()
            bundle.append(copy)
        loads.append(bundle)

    barrier = pltpu.get_barrier_semaphore()
    for peer in (along_x, along_y, {"seq": mate}):
        pl.semaphore_signal(barrier, inc=1, device_id=peer, device_id_type=MESH)

    @pl.when(has_up)
    def _():
        pl.semaphore_signal(barrier, inc=1, device_id={"seq": s + 2}, device_id_type=MESH)

    @pl.when(has_down)
    def _():
        pl.semaphore_signal(barrier, inc=1, device_id={"seq": s - 2}, device_id_type=MESH)

    pl.semaphore_wait(barrier, 3 + has_up.astype(jnp.int32) + has_down.astype(jnp.int32))

    moves = []
    for part in range(2):
        top, bottom = pl.ds(part * half, quarter), pl.ds(part * half + quarter, quarter)
        spec = (
            (x_ref.at[top], buf.at[0, top], along_x),
            (x_ref.at[bottom], buf.at[1, bottom], along_y),
            (x_ref.at[bottom], buf.at[0, bottom], along_x),
            (x_ref.at[top], buf.at[1, top], along_y),
            (buf.at[0, top], buf.at[2, top], along_y),
            (buf.at[1, bottom], buf.at[2, bottom], along_x),
        )
        moves.append(
            [
                remote(source, target, send.at[part * 6 + i], recv.at[part * 6 + i], device)
                for i, (source, target, device) in enumerate(spec)
            ]
        )

    def begin_gather(part):
        for i in range(4):
            moves[part][i].start()

    def pass_on(part):
        moves[part][0].wait_recv()
        moves[part][4].start()
        moves[part][1].wait_recv()
        moves[part][5].start()

    def up(owner, part, source):
        index = owner * 2 + part
        return remote(
            source, kv_buf.at[index], up_sem.at[index], kv_sem.at[index], {"seq": s + 2}
        )

    def side(owner, part, source):
        index = owner * 2 + part
        return remote(
            source, kv_buf.at[index], side_sem.at[index], kv_sem.at[index], {"seq": mate}
        )

    def arrive(owner, part):
        block = kv_buf.at[owner * 2 + part]
        up(owner, part, block).wait_recv()

        @pl.when(has_up)
        def _():
            up(owner, part, block).start()

        side(owner, part, block).start()

    tile = 256 if total % 256 == 0 else 128
    step_rows = 64 if half % 64 == 0 else half

    def take(slot, part, source):
        gain_span = pl.ds(pl.multiple_of(owners[slot] * cols, cols), cols)

        def prepare(i, carry):
            here = pl.ds(pl.multiple_of(i * step_rows, step_rows), step_rows)
            there = pl.ds(pl.multiple_of(part * half + i * step_rows, step_rows), step_rows)
            wide = source[there, :].astype(F32)
            squares = jnp.sum(wide * wide, axis=-1, keepdims=True)
            spread = jnp.broadcast_to(squares, (step_rows, HEAD_DIM))
            if slot == 0:
                ss[here, :] = spread
            else:
                ss[here, :] += spread
            xg[here, :] = (wide * gain_ref[:, gain_span]).astype(BF16)
            return carry

        lax.fori_loop(0, half // step_rows, prepare, 0)
        if part == 0:
            for copy in loads[slot]:
                copy.wait()

        def multiply(j, carry):
            span = pl.ds(pl.multiple_of(j * tile, tile), tile)
            product = jnp.dot(xg[...], w[slot, :, span], preferred_element_type=F32)
            if slot == 0:
                acc[:, span] = product
            else:
                acc[:, span] += product
            return carry

        lax.fori_loop(0, total // tile, multiply, 0)

    def finish_part(part):
        factor = lax.rsqrt(ss[...] * (1.0 / D) + NORM_EPS)
        span = pl.ds(part * half, half)

        def rotated(index):
            u = acc[:, pl.ds(index * HEAD_DIM, HEAD_DIM)] * factor
            turned = pltpu.roll(u, HEAD_DIM // 2, 1)
            return (u * cos_ref[span, :] + turned * sin_ref[span, :]).astype(BF16)

        for h in range(kv_heads):
            kv_own[part, 0, h] = rotated(heads + h)
            place = (heads + kv_heads + h) * HEAD_DIM
            kv_own[part, 1, h] = (acc[:, pl.ds(place, HEAD_DIM)] * factor).astype(BF16)
        for h in range(heads):
            q_all[h, span] = rotated(h)

        @pl.when(has_up)
        def _():
            up(s, part, kv_own.at[part]).start()

        @pl.when(c == 0)
        def _():
            side(s, part, kv_own.at[part]).start()

    begin_gather(0)
    take(0, 0, x_ref)
    pass_on(0)
    begin_gather(1)
    moves[0][2].wait_recv()
    take(1, 0, buf.at[0])
    moves[0][3].wait_recv()
    take(2, 0, buf.at[1])
    moves[0][4].wait_recv()
    moves[0][5].wait_recv()
    take(3, 0, buf.at[2])
    finish_part(0)
    pass_on(1)
    take(0, 1, x_ref)
    moves[1][2].wait_recv()
    take(1, 1, buf.at[0])
    moves[1][3].wait_recv()
    take(2, 1, buf.at[1])

    @pl.when(has_down)
    def _():
        arrive(s - 2, 0)

    moves[1][4].wait_recv()
    moves[1][5].wait_recv()
    take(3, 1, buf.at[2])
    finish_part(1)

    for part in range(2):
        shift = part * half

        def own(h, carry):
            attend(
                q_all, kv_own[part, 0, h], kv_own[part, 1, h], out, lsum, h, group,
                lambda row, col: col + shift <= row, part == 0,
            )
            return carry

        lax.fori_loop(0, kv_heads, own, 0)

    def visit(owner, part):
        index = owner * 2 + part

        def body(h, carry):
            attend(
                q_all, kv_buf[index, 0, h], kv_buf[index, 1, h], out, lsum, h, group, None, False
            )
            return carry

        lax.fori_loop(0, kv_heads, body, 0)

    @pl.when(z > 0)
    def _():
        arrive(s - 2, 1)

    @pl.when(c == 1)
    def _():
        for part in range(2):
            side(s - 1, part, kv_buf.at[(s - 1) * 2 + part]).wait_recv()
            visit(s - 1, part)

    def level(unit, carry):
        k, part = 1 + unit // 2, unit % 2
        owner, other = s - 2 * k, mate - 2 * k

        @pl.when(unit >= 2)
        def _():
            arrive(owner, part)

        visit(owner, part)
        side(other, part, kv_buf.at[other * 2 + part]).wait_recv()
        visit(other, part)
        return carry

    lax.fori_loop(0, 2 * z, level, 0)
    write_heads(o_ref, out, lsum)

    for part in range(2):
        for copy in moves[part]:
            copy.wait_send()

        @pl.when(has_up)
        def _():
            up(s, part, kv_own.at[part]).wait_send()

        @pl.when(c == 0)
        def _():
            side(s, part, kv_own.at[part]).wait_send()

    def drain(unit, carry):
        owner, part = s - 2 * (1 + unit // 2), unit % 2
        block = kv_buf.at[owner * 2 + part]

        @pl.when(has_up)
        def _():
            up(owner, part, block).wait_send()

        side(owner, part, block).wait_send()
        return carry

    lax.fori_loop(0, 2 * z, drain, 0)


def front(x, gain, cos, sin, wq, wk, wv, count, collective_id):
    rows, cols = x.shape
    half = rows // 2
    heads, kv_heads = wq.shape[1] // HEAD_DIM, wk.shape[1] // HEAD_DIM
    total = wq.shape[1] + 2 * wk.shape[1]
    vmem = pl.BlockSpec(memory_space=VMEM)
    hbm = pl.BlockSpec(memory_space=pl.ANY)
    return pl.pallas_call(
        functools.partial(front_kernel, count // 2, heads, kv_heads),
        out_shape=jax.ShapeDtypeStruct((rows, heads * HEAD_DIM), BF16),
        in_specs=[vmem] * 4 + [hbm] * 3,
        out_specs=vmem,
        scratch_shapes=[
            VMEM((3, rows, cols), BF16),
            VMEM((half, cols), BF16),
            VMEM((4, cols, total), BF16),
            VMEM((half, total), F32),
            VMEM((half, HEAD_DIM), F32),
            VMEM((heads, rows, HEAD_DIM), BF16),
            VMEM((2, 2, kv_heads, half, HEAD_DIM), BF16),
            VMEM((2 * count, 2, kv_heads, half, HEAD_DIM), BF16),
            VMEM((heads, rows, HEAD_DIM), F32),
            VMEM((heads, rows, HEAD_DIM), F32),
            pltpu.SemaphoreType.DMA((12,)),
            pltpu.SemaphoreType.DMA((12,)),
            pltpu.SemaphoreType.DMA((4, 3)),
            pltpu.SemaphoreType.DMA((2 * count,)),
            pltpu.SemaphoreType.DMA((2 * count,)),
            pltpu.SemaphoreType.DMA((2 * count,)),
        ],
        compiler_params=pltpu.CompilerParams(
            collective_id=collective_id, has_side_effects=True, vmem_limit_bytes=48 * 2**20
        ),
        name="front",
    )(x, gain[None, :], cos, sin, wq, wk, wv)


def output_kernel(
    a_ref, tok_ref, gain_ref, wo_ref, hidden_ref,
    wbuf, part, own, landed, passed, mine, stats, wsem, send, recv, ssend, srecv,
):
    me = lax.axis_index("tp")
    rows, cols = tok_ref.shape
    half = rows // 2
    owners = [xor(me, bits) for bits in range(4)]
    peers = [{"tp": owner} for owner in owners]
    order = (3, 1, 2, 0)
    loads = []
    for slot, bits in enumerate(order):
        span = pl.ds(pl.multiple_of(owners[bits] * cols, cols), cols)
        copy = pltpu.make_async_copy(wo_ref.at[:, span], wbuf.at[slot], wsem.at[slot])
        copy.start()
        loads.append(copy)
    greet(peers[1:])
    top, bottom = pl.ds(0, half), pl.ds(half, half)
    diag_x = remote(part.at[0, top], landed.at[0], send.at[0], recv.at[0], peers[1])
    diag_y = remote(part.at[0, bottom], landed.at[1], send.at[1], recv.at[1], peers[2])
    last_x_top = remote(part.at[1, top], landed.at[2], send.at[2], recv.at[2], peers[1])
    last_y_bottom = remote(part.at[2, bottom], landed.at[3], send.at[3], recv.at[3], peers[2])
    last_x_bottom = remote(passed.at[1], landed.at[4], send.at[4], recv.at[4], peers[1])
    last_y_top = remote(passed.at[0], landed.at[5], send.at[5], recv.at[5], peers[2])

    tile = 384 if cols % 384 == 0 else 128

    def product(slot, store):
        loads[slot].wait()

        def body(j, carry):
            span = pl.ds(pl.multiple_of(j * tile, tile), tile)
            store(span, jnp.dot(a_ref[...], wbuf[slot, :, span], preferred_element_type=F32))
            return carry

        lax.fori_loop(0, cols // tile, body, 0)

    def store_part(slot):
        def store(span, value):
            part[slot, :, span] = value.astype(BF16)

        return store

    def store_own(span, value):
        own[:, span] = value

    product(0, store_part(0))
    diag_x.start()
    diag_y.start()
    product(1, store_part(1))
    last_x_top.start()
    product(2, store_part(2))
    last_y_bottom.start()
    product(3, store_own)
    diag_x.wait_recv()
    passed[0] = (part[2, 0:half].astype(F32) + landed[0].astype(F32)).astype(BF16)
    last_y_top.start()
    diag_y.wait_recv()
    passed[1] = (part[1, half:rows].astype(F32) + landed[1].astype(F32)).astype(BF16)
    last_x_bottom.start()
    last_x_top.wait_recv()
    own[0:half] += landed[2].astype(F32)
    last_y_bottom.wait_recv()
    own[half:rows] += landed[3].astype(F32)
    last_y_top.wait_recv()
    own[0:half] += landed[5].astype(F32)
    last_x_bottom.wait_recv()
    own[half:rows] += landed[4].astype(F32)

    lanes = jnp.zeros((rows, HEAD_DIM), F32)
    for begin in range(0, cols, HEAD_DIM):
        piece = own[:, begin : begin + HEAD_DIM]
        lanes = lanes + piece * piece
    ones = jnp.ones((8, HEAD_DIM), F32)
    highest = lax.Precision.HIGHEST
    mine[...] = lax.dot_general(
        ones, lanes, (((1,), (1,)), ((), ())), precision=highest, preferred_element_type=F32
    )
    swaps = []
    for bits in (3, 1, 2):
        swap = remote(mine, stats.at[bits - 1], ssend.at[bits - 1], srecv.at[bits - 1], peers[bits])
        swap.start()
        swaps.append(swap)
    for swap in swaps:
        swap.wait_recv()
    summed = mine[...] + stats[0] + stats[1] + stats[2]
    column = lax.dot_general(
        summed, ones * 0.125, (((0,), (0,)), ((), ())), precision=highest,
        preferred_element_type=F32,
    )
    factor = lax.rsqrt(column * (1.0 / D) + NORM_EPS)
    span = pl.multiple_of(me * cols, cols)
    for begin in range(0, cols, HEAD_DIM):
        stop = begin + HEAD_DIM
        gain = gain_ref[:, pl.ds(pl.multiple_of(span + begin, HEAD_DIM), HEAD_DIM)]
        hidden_ref[:, begin:stop] = (
            tok_ref[:, begin:stop].astype(F32) + own[:, begin:stop] * factor * gain
        ).astype(BF16)
    for copy in (diag_x, diag_y, last_x_top, last_y_bottom, last_x_bottom, last_y_top, *swaps):
        copy.wait_send()


def output_project(attended, tokens, gain, wo, collective_id):
    rows, cols = tokens.shape
    depth = attended.shape[1]
    vmem = pl.BlockSpec(memory_space=VMEM)
    return pl.pallas_call(
        output_kernel,
        out_shape=jax.ShapeDtypeStruct((rows, cols), BF16),
        in_specs=[vmem] * 3 + [pl.BlockSpec(memory_space=pl.ANY)],
        out_specs=vmem,
        scratch_shapes=[
            VMEM((4, depth, cols), BF16),
            VMEM((3, rows, cols), BF16),
            VMEM((rows, cols), F32),
            VMEM((6, rows // 2, cols), BF16),
            VMEM((2, rows // 2, cols), BF16),
            VMEM((8, rows), F32),
            VMEM((3, 8, rows), F32),
            pltpu.SemaphoreType.DMA((4,)),
            pltpu.SemaphoreType.DMA((6,)),
            pltpu.SemaphoreType.DMA((6,)),
            pltpu.SemaphoreType.DMA((3,)),
            pltpu.SemaphoreType.DMA((3,)),
        ],
        compiler_params=pltpu.CompilerParams(
            collective_id=collective_id, has_side_effects=True, vmem_limit_bytes=40 * 2**20
        ),
        name="output_project",
    )(attended, tokens, gain[None, :], wo)


def window_kernel(count, q_ref, kv_ref, o_ref, tail, acc, lsum, send, recv):
    s = lax.axis_index("seq")
    kv_heads, rows = kv_ref.shape[1], kv_ref.shape[2]
    group = q_ref.shape[0] // kv_heads
    has_next, has_last = s < count - 1, s > 0
    barrier = pltpu.get_barrier_semaphore()

    @pl.when(has_next)
    def _():
        pl.semaphore_signal(barrier, inc=1, device_id={"seq": s + 1}, device_id_type=MESH)

    @pl.when(has_last)
    def _():
        pl.semaphore_signal(barrier, inc=1, device_id={"seq": s - 1}, device_id_type=MESH)

    pl.semaphore_wait(barrier, has_next.astype(jnp.int32) + has_last.astype(jnp.int32))
    copy = remote(
        kv_ref.at[:, :, pl.ds(rows - WINDOW, WINDOW), :], tail, send.at[0], recv.at[0],
        {"seq": s + 1},
    )

    @pl.when(has_next)
    def _():
        copy.start()

    def own(h, carry):
        attend(
            q_ref, kv_ref[0, h], kv_ref[1, h], acc, lsum, h, group,
            lambda row, col: (col <= row) & (row - col < WINDOW), True,
        )
        return carry

    lax.fori_loop(0, kv_heads, own, 0)

    @pl.when(has_last)
    def _():
        copy.wait_recv()

        def body(h, carry):
            attend(
                q_ref, tail[0, h], tail[1, h], acc, lsum, h, group,
                lambda row, col: col > row, False, (0, WINDOW),
            )
            return carry

        lax.fori_loop(0, kv_heads, body, 0)

    write_heads(o_ref, acc, lsum)

    @pl.when(has_next)
    def _():
        copy.wait_send()


def window_attention(q, kv, count, collective_id):
    heads, rows, _ = q.shape
    vmem = pl.BlockSpec(memory_space=VMEM)
    return pl.pallas_call(
        functools.partial(window_kernel, count),
        out_shape=jax.ShapeDtypeStruct((rows, heads * HEAD_DIM), BF16),
        in_specs=[vmem] * 2,
        out_specs=vmem,
        scratch_shapes=[
            VMEM((2, kv.shape[1], WINDOW, HEAD_DIM), BF16),
            VMEM(q.shape, F32),
            VMEM(q.shape, F32),
            pltpu.SemaphoreType.DMA((1,)),
            pltpu.SemaphoreType.DMA((1,)),
        ],
        compiler_params=pltpu.CompilerParams(
            collective_id=collective_id, has_side_effects=True, vmem_limit_bytes=24 * 2**20
        ),
        name="window_attention",
    )(q, kv)


def rms_scaled(values, weights):
    widened = values.astype(F32)
    factor = lax.rsqrt(jnp.mean(widened * widened, axis=-1, keepdims=True) + NORM_EPS)
    return widened * factor * weights


def plain_gather_project(x, gain, cos, sin, wq, wk, wv):
    full = lax.all_gather(x, "tp", axis=1, tiled=True)
    normed = rms_scaled(full, gain).astype(BF16)

    def heads_of(weight):
        product = jnp.dot(normed, weight, preferred_element_type=F32)
        return jnp.swapaxes(product.reshape(x.shape[0], -1, HEAD_DIM), 0, 1)

    def rotated(u):
        return (u * cos + jnp.roll(u, HEAD_DIM // 2, axis=-1) * sin).astype(BF16)

    keys, values = rotated(heads_of(wk)), heads_of(wv).astype(BF16)
    return rotated(heads_of(wq)), jnp.stack([keys, values])


def plain_output_project(attended, tokens, gain, wo):
    cols = tokens.shape[1]
    partial_sum = jnp.dot(attended, wo, preferred_element_type=F32).astype(BF16)
    summed = lax.psum(partial_sum, "tp").astype(F32)
    added = rms_scaled(summed, gain)
    mine = lax.dynamic_slice_in_dim(added, lax.axis_index("tp") * cols, cols, 1)
    return (tokens.astype(F32) + mine).astype(BF16)


def local(
    sizes,
    tokens,
    attention_gain,
    query_weight,
    key_weight,
    value_weight,
    output_weight,
    post_gain,
    local_gain,
    local_query_weight,
    local_key_weight,
    local_value_weight,
):
    seq, tp = sizes
    rows, cols = tokens.shape
    places = lax.axis_index("seq") * rows + lax.iota(jnp.int32, rows)
    halfway = HEAD_DIM // 2
    exponents = jnp.arange(halfway, dtype=F32) * (2.0 / HEAD_DIM)
    frequency = jnp.power(F32(10000.0), -exponents)
    angles = places.astype(F32)[:, None] * frequency[None, :]
    cosine, sine = jnp.cos(angles), jnp.sin(angles)
    cos = jnp.concatenate([cosine, cosine], axis=-1)
    sin = jnp.concatenate([-sine, sine], axis=-1)
    square = tp == 4 and cols % HEAD_DIM == 0

    def project(x, gain, wq, wk, wv, collective_id):
        if square:
            return gather_project(x, gain, cos, sin, wq, wk, wv, collective_id)
        return plain_gather_project(x, gain, cos, sin, wq, wk, wv)

    first = (tokens, attention_gain, cos, sin, query_weight, key_weight, value_weight)
    if square:
        attended = front(*first, seq, 0)
        hidden = output_project(attended, tokens, post_gain, output_weight, 2)
    else:
        attended = causal_attention(*plain_gather_project(*first), seq, 1)
        hidden = plain_output_project(attended, tokens, post_gain, output_weight)
    lq, lkv = project(
        hidden, local_gain, local_query_weight, local_key_weight, local_value_weight, 3
    )
    return hidden, window_attention(lq, lkv, seq, 4)


def solution(mesh):
    in_specs = (
        P("seq", "tp"),
        P(),
        P(None, "tp"),
        P(None, "tp"),
        P(None, "tp"),
        P("tp", None),
        P(),
        P(),
        P(None, "tp"),
        P(None, "tp"),
        P(None, "tp"),
    )
    out_specs = (P("seq", "tp"), P("seq", "tp"))
    sizes = (mesh.shape["seq"], mesh.shape["tp"])
    body = functools.partial(local, sizes)
    return jax.shard_map(body, mesh=mesh, in_specs=in_specs, out_specs=out_specs, check_vma=False)
```
